32 devices in a mesh: coil: 4 (over x, core), slab: 8 (over z, y).
Axes of the slice: x: 2, y: 2, z: 4, core: 2. Of those that a mesh axis runs over, the one named last changes fastest.
Arguments:
- kspace_data: bfloat16 [32, 2, 128, 128, 128], P('coil', None, None, 'slab'), may hold values from -4 to 4
- coil_maps: bfloat16 [32, 2, 128, 128, 128], P('coil', None, 'slab'), may hold values from -1.796875 to 1.796875
- sample_mask: int32 [32, 128, 128], P('coil', None, 'slab'), may hold values 0 or 1
- initial_image: float32 [2, 128, 128, 128], P(None, 'slab', 'coil'), may hold values from -6 to 6
Outputs:
- image: float32 [2, 128, 128, 128], P(None, 'slab', 'coil')
The draws below stay inside these ranges and needn't reach their ends.
All inputs are finite; a program needn't handle non-finite values. No bound on the sum of `sample_mask` on one device may be relied on, other than what follows from the above.
Results may differ from the reference program's by a relative error of at most 0.0045.
Values may be sent and summed in bfloat16 or wider, within the bound.
A program may use at most 128 MiB of HBM per device.

```python
import math
import jax
import jax.numpy as jnp
from jax import lax

NX = 128
NY = 128
NZ = 128
COILS = 32
ITERS = 2


def touch_ends(entries, own_key, smallest, top_value):
    dims = entries.shape
    spot = [jax.random.randint(jax.random.fold_in(own_key, axis), (), 0, dims[axis]) for axis in range(len(dims))]
    entries = entries.at[tuple(spot)].set(smallest)
    longest = dims.index(max(dims))
    spot[longest] = (spot[longest] + 1) % dims[longest]
    return entries.at[tuple(spot)].set(top_value)


def spiked(entries, rng, source, target, blocks, factor):
    owner, partner = [(jnp.arange(entries.shape[axis_at]) // (entries.shape[axis_at] // blocks)).reshape([-1 if axis == axis_at else 1 for axis in range(entries.ndim)]) for axis_at in (source, target)]
    chosen = jax.random.permutation(rng, blocks)[partner]
    strong = (owner == chosen) | (owner == (partner + blocks // 2) % blocks)
    return jnp.where(strong, factor * entries, entries)


def block_scale(stream_key, dims, cuts, low, high):
    loudness = 1.0
    for position, shards_of in cuts:
        heights = jax.random.uniform(jax.random.fold_in(jax.random.fold_in(stream_key, 6), position), (shards_of,), jnp.float32, low / len(cuts), high / len(cuts))
        loudness = loudness * jnp.repeat(jnp.exp(heights), dims[position] // shards_of).reshape((-1,) + (1,) * (len(dims) - 1 - position))
    return loudness


def normal_values(stream_key, shape, scale, limit, cuts=(), kind=jnp.bfloat16):
    level = block_scale(stream_key, shape, cuts, -0.22, 0.18) if cuts else 1.0
    entries = jax.random.normal(stream_key, shape, jnp.float32) * scale * level
    return jnp.minimum(jnp.maximum(entries, -limit), limit).astype(kind)


def bell_draw_with(rng, shape, scale, bound, cuts, heavy, kind=jnp.bfloat16):
    array = scale * jax.random.normal(rng, shape, jnp.float32)
    if cuts:
        array = array * block_scale(rng, shape, cuts, -0.22, 0.18)
    return jnp.clip(spiked(array, jax.random.fold_in(rng, 3), *heavy), -bound, bound).astype(kind)


def setup_inputs(seed: int = 0) -> dict:
    key_list = jax.random.split(jax.random.key(seed), 5)
    kspace_data = normal_values(key_list[0], (COILS, 2, NZ, NY, NX), 0.5, 4.0, ((0, 4), (3, 8)))
    coil_maps = bell_draw_with(key_list[1], (COILS, 2, NZ, NY, NX), 0.3, 1.796875, ((0, 4), (2, 8)), (0, 3, 4, 2.0))
    sample_mask = touch_ends((jax.random.randint(key_list[2], (COILS, NZ, NY), 0, 3) < 1).astype(jnp.int32), jax.random.fold_in(key_list[2], 1), 0, 1)
    initial_image = normal_values(key_list[3], (2, NZ, NY, NX), 1.0, 6.0, ((1, 8), (2, 4)), jnp.float32)
    return {"kspace_data": kspace_data, "coil_maps": coil_maps, "sample_mask": sample_mask, "initial_image": initial_image}


dual_step = 0.25
primal_step = 0.25
tv_weight = 0.5

def dft_table(length, inverse):
    counter = jnp.arange(length, dtype=jnp.int32)
    product = counter[:, None] * counter[None, :] % length
    phase = 2.0 * math.pi / length * product.astype(jnp.float32)
    scale = 1.0 / math.sqrt(length)
    real_part = jnp.cos(phase) * scale
    imag_part = jnp.sin(phase) * scale
    if not inverse:
        imag_part = -imag_part
    table = jnp.stack([jnp.stack([real_part, imag_part]), jnp.stack([-imag_part, real_part])])
    return table.astype(jnp.bfloat16)

def along_x(field, table):
    return jnp.einsum('kzyx,kjxw->jzyw', field.astype(jnp.float32), table.astype(jnp.float32))

def along_y(field, table):
    return jnp.einsum('kzyx,kjyv->jzvx', field.astype(jnp.float32), table.astype(jnp.float32))

def along_z(field, table):
    return jnp.einsum('kzyx,kjzw->jwyx', field.astype(jnp.float32), table.astype(jnp.float32))

def forward_diff(field, axis_pos):
    length = field.shape[axis_pos]
    upper = lax.slice_in_dim(field, 1, length, axis=axis_pos)
    lower = lax.slice_in_dim(field, 0, length - 1, axis=axis_pos)
    zero_slice = jnp.zeros_like(lax.slice_in_dim(field, 0, 1, axis=axis_pos))
    return jnp.concatenate([upper - lower, zero_slice], axis_pos)

def backward_diff(field, axis_pos):
    length = field.shape[axis_pos]
    lower = lax.slice_in_dim(field, 0, length - 1, axis=axis_pos)
    zero_slice = jnp.zeros_like(lax.slice_in_dim(field, 0, 1, axis=axis_pos))
    return jnp.concatenate([zero_slice, lower], axis_pos) - field

def reference(kspace_data, coil_maps, sample_mask, initial_image):
    forward_x = dft_table(NX, False)
    forward_y = dft_table(NY, False)
    forward_z = dft_table(NZ, False)
    inverse_x = dft_table(NX, True)
    inverse_y = dft_table(NY, True)
    inverse_z = dft_table(NZ, True)
    current = initial_image
    guess = initial_image
    dual_data = jnp.zeros(kspace_data.shape, jnp.float32)
    duals = (jnp.zeros_like(current), jnp.zeros_like(current), jnp.zeros_like(current))
    for turn_index in range(ITERS):

        def per_coil(total, items):
            maps_one, data_one, mask_one, dual_one = items
            maps_real = maps_one[0].astype(jnp.float32)
            maps_imag = maps_one[1].astype(jnp.float32)
            pieces = jnp.stack([maps_real * guess[0] - maps_imag * guess[1], maps_real * guess[1] + maps_imag * guess[0]]).astype(jnp.bfloat16)
            pieces = along_x(pieces, forward_x).astype(jnp.bfloat16)
            pieces = along_y(pieces, forward_y).astype(jnp.bfloat16)
            spectrum = along_z(pieces, forward_z)
            sampled = mask_one[None, :, :, None].astype(jnp.float32)
            dual_new = (dual_one + dual_step * (sampled * (spectrum - data_one.astype(jnp.float32)))) / (1.0 + dual_step)
            back_field = along_z(dual_new.astype(jnp.bfloat16), inverse_z).astype(jnp.bfloat16)
            back_field = along_y(back_field, inverse_y).astype(jnp.bfloat16)
            back_field = along_x(back_field, inverse_x)
            combined = jnp.stack([maps_real * back_field[0] + maps_imag * back_field[1], maps_real * back_field[1] - maps_imag * back_field[0]])
            return (total + combined, dual_new)
        data_grad, dual_data = lax.scan(per_coil, jnp.zeros_like(current), (coil_maps, kspace_data, sample_mask, dual_data))
        grads = (forward_diff(guess, 1), forward_diff(guess, 2), forward_diff(guess, 3))
        moved = [duals[num] + dual_step * grads[num] for num in range(3)]
        magnitude = jnp.sqrt(lax.optimization_barrier(jnp.sum(moved[0] * moved[0], 0)) + lax.optimization_barrier(jnp.sum(moved[1] * moved[1], 0)) + lax.optimization_barrier(jnp.sum(moved[2] * moved[2], 0)))
        factor = 1.0 / jnp.maximum(1.0, magnitude / tv_weight)
        duals = (moved[0] * factor, moved[1] * factor, moved[2] * factor)
        spread = backward_diff(duals[0], 1) + backward_diff(duals[1], 2) + backward_diff(duals[2], 3)
        updated = current - primal_step * (data_grad + spread)
        guess = 2.0 * updated - current
        current = updated
    return current
```

```python
import functools
import math

import jax
import jax.numpy as jnp
import ml_dtypes
import numpy as np
from jax import lax
from jax.experimental import pallas as pl
from jax.experimental.pallas import tpu as pltpu
from jax.sharding import PartitionSpec as P

ITERS = 2

dual_step = 0.25
primal_step = 0.25
tv_weight = 0.5
f32 = jnp.float32
bf16 = jnp.bfloat16


def from_behind(block, axis, distance):
    devices = range(lax.axis_size(axis))
    route = [(i - distance, i) for i in devices if i - distance in devices]
    return lax.ppermute(block, axis, route)


def dft_table(length, inverse):
    counter = np.arange(length)
    phase = 2.0 * math.pi / length * (np.outer(counter, counter) % length)
    real_part = np.cos(phase) / math.sqrt(length)
    imag_part = np.sin(phase) / math.sqrt(length)
    if not inverse:
        imag_part = -imag_part
    table = np.stack([np.stack([real_part, imag_part]), np.stack([-imag_part, real_part])])
    return table.astype(ml_dtypes.bfloat16)


def on_right(table):
    n = table.shape[2]
    return jnp.asarray(table.transpose(0, 2, 1, 3).reshape(2 * n, 2 * n))


def on_left(table):
    n = table.shape[2]
    return jnp.asarray(table.transpose(1, 3, 0, 2).reshape(2 * n, 2 * n))


def plane(ref, coil, part):
    block = ref[:, coil, 0, part]
    return block.reshape(block.shape[0] * block.shape[1], block.shape[2])


def dot(a, b, dims=((1,), (0,))):
    return lax.dot_general(a, b, (dims, ((), ())), preferred_element_type=f32)


def combine(out_ref, maps_ref, images, group):
    nz, ny = out_ref.shape[2:]
    real_sum = imag_sum = None
    for coil in range(group):
        real = images[coil * nz : (coil + 1) * nz, :ny]
        imag = images[coil * nz : (coil + 1) * nz, ny:]
        maps_real = plane(maps_ref, coil, 0).astype(f32)
        maps_imag = plane(maps_ref, coil, 1).astype(f32)
        real_term = maps_real * real + maps_imag * imag
        imag_term = maps_real * imag - maps_imag * real
        real_sum = real_term if coil == 0 else real_sum + real_term
        imag_sum = imag_term if coil == 0 else imag_sum + imag_term

    @pl.when(pl.program_id(1) == 0)
    def _():
        out_ref[0, 0] = real_sum
        out_ref[0, 1] = imag_sum

    @pl.when(pl.program_id(1) > 0)
    def _():
        out_ref[0, 0] += real_sum
        out_ref[0, 1] += imag_sum


def normal_kernel(group, guess_ref, maps_ref, mask_ref, fy_ref, fz_ref, gz_ref, gy_ref, out_ref):
    nz, ny = out_ref.shape[2:]
    guess_real = guess_ref[0, 0]
    guess_imag = guess_ref[0, 1]
    rows = []
    for coil in range(group):
        maps_real = plane(maps_ref, coil, 0).astype(f32)
        maps_imag = plane(maps_ref, coil, 1).astype(f32)
        real = maps_real * guess_real - maps_imag * guess_imag
        imag = maps_real * guess_imag + maps_imag * guess_real
        rows.append(jnp.concatenate([real.astype(bf16), imag.astype(bf16)], 1))
    pieces = dot(jnp.concatenate(rows, 0), fy_ref[...]).astype(bf16)
    pieces = jnp.concatenate(
        [
            jnp.concatenate(
                [pieces[c * nz : (c + 1) * nz, j * ny : (j + 1) * ny] for c in range(group)], 1
            )
            for j in range(2)
        ],
        0,
    )
    spectrum = dot(fz_ref[...], pieces).astype(bf16)
    mask = jnp.concatenate([mask_ref[c] for c in range(group)], 1)
    spectrum = spectrum * jnp.concatenate([mask, mask], 0)
    pieces = dot(gz_ref[...], spectrum).astype(bf16)
    pieces = jnp.concatenate(
        [
            jnp.concatenate(
                [pieces[j * nz : (j + 1) * nz, c * ny : (c + 1) * ny] for j in range(2)], 1
            )
            for c in range(group)
        ],
        0,
    )
    combine(out_ref, maps_ref, dot(pieces, gy_ref[...]), group)


def data_kernel(group, data_ref, maps_ref, gy_ref, out_ref):
    columns = jnp.concatenate(
        [
            jnp.concatenate([plane(data_ref, c, 0), plane(data_ref, c, 1)], 0)
            for c in range(group)
        ],
        1,
    )
    combine(out_ref, maps_ref, dot(columns, gy_ref[...], ((0,), (0,))), group)


def whole(shape):
    return pl.BlockSpec(shape, lambda x, c: (0,) * len(shape))


def coil_blocks(array, group):
    src, _, _, parts, planes, cols = array.shape
    return pl.BlockSpec((src, group, 1, parts, planes, cols), lambda x, c: (0, c, x, 0, 0, 0))


def call(kernel, group, operands, specs, shape, coils, flops, nbytes):
    return pl.pallas_call(
        functools.partial(kernel, group),
        out_shape=jax.ShapeDtypeStruct(shape, f32),
        grid=(shape[0], coils // group),
        in_specs=specs,
        out_specs=pl.BlockSpec((1,) + shape[1:], lambda x, c: (x, 0, 0, 0)),
        compiler_params=pltpu.CompilerParams(
            dimension_semantics=("arbitrary", "arbitrary"), vmem_limit_bytes=48 * 2**20
        ),
        cost_estimate=pl.CostEstimate(flops=flops, bytes_accessed=nbytes, transcendentals=0),
    )(*operands)


def coil_group(coils):
    return max(g for g in (1, 2, 4) if coils % g == 0)


def apply_normal(guess, maps, mask, tables):
    coils = maps.shape[1]
    group = coil_group(coils)
    shape = guess.shape
    specs = [
        pl.BlockSpec((1,) + shape[1:], lambda x, c: (x, 0, 0, 0)),
        coil_blocks(maps, group),
        pl.BlockSpec((group,) + mask.shape[1:], lambda x, c: (c, 0, 0)),
    ] + [whole(t.shape) for t in tables]
    cells = coils * shape[0] * shape[2] * shape[3]
    return call(
        normal_kernel, group, (guess, maps, mask) + tables, specs, shape, coils, cells * 4096, cells * 4
    )


def apply_data(data, maps, table, shape):
    coils = maps.shape[1]
    group = coil_group(coils)
    specs = [coil_blocks(data, group), coil_blocks(maps, group), whole(table.shape)]
    cells = coils * shape[0] * shape[2] * shape[3]
    return call(data_kernel, group, (data, maps, table), specs, shape, coils, cells * 1024, cells * 8)


def exchange(blocks):
    got = lax.all_to_all(blocks, "slab", split_axis=0, concat_axis=0, tiled=True)
    if got.shape[4] % 16:
        src, coils, width, parts, share, cols = got.shape
        got = got.transpose(1, 2, 3, 0, 4, 5).reshape(1, coils, width, parts, src * share, cols)
    return got


def tv_update(guess, duals):
    width = guess.shape[0]
    size = lax.axis_size("slab") * width
    pos = lax.axis_index("slab") * width + lax.broadcasted_iota(jnp.int32, (width, 1, 1, 1), 0)
    ahead_x = jnp.concatenate([guess[1:], from_behind(guess[:1], "slab", -1)], 0)
    grad_x = jnp.where(pos < size - 1, ahead_x - guess, 0.0)
    grad_z = jnp.concatenate(
        [guess[:, :, 1:] - guess[:, :, :-1], jnp.zeros_like(guess[:, :, :1])], 2
    )
    grad_y = jnp.concatenate([guess[..., 1:] - guess[..., :-1], jnp.zeros_like(guess[..., :1])], 3)
    moved = [dual_step * grad for grad in (grad_z, grad_y, grad_x)]
    if duals is not None:
        moved = [dual + step for dual, step in zip(duals, moved)]
    magnitude = jnp.sqrt(sum(jnp.sum(w * w, 1, keepdims=True) for w in moved))
    factor = 1.0 / jnp.maximum(1.0, magnitude / tv_weight)
    dual_z, dual_y, dual_x = [w * factor for w in moved]
    prior = from_behind(dual_x[-1:], "slab", 1)
    spread_x = jnp.concatenate([prior, dual_x[:-1]], 0) - dual_x
    spread_z = jnp.concatenate([jnp.zeros_like(dual_z[:, :, :1]), dual_z[:, :, :-1]], 2) - dual_z
    spread_y = jnp.concatenate([jnp.zeros_like(dual_y[..., :1]), dual_y[..., :-1]], 3) - dual_y
    return (dual_z, dual_y, dual_x), spread_z + spread_y + spread_x


def on_device(kspace_data, coil_maps, sample_mask, initial_image):
    slabs = lax.axis_size("slab")
    groups = lax.axis_size("coil")
    coils, _, planes, ny, nx = coil_maps.shape
    nz = kspace_data.shape[2]
    shares = kspace_data.shape[3]
    rows = initial_image.shape[2]
    width = nx // slabs
    forward_y, inverse_y = dft_table(ny, False), dft_table(ny, True)
    forward_z, inverse_z = dft_table(nz, False), dft_table(nz, True)
    inverse_x = jnp.asarray(dft_table(nx, True))
    tables = (on_right(forward_y), on_left(forward_z), on_left(inverse_z), on_right(inverse_y))

    image = initial_image.reshape(2, planes, rows, slabs, width).transpose(3, 4, 0, 2, 1)
    image = lax.all_to_all(
        image.reshape(slabs, -1), "slab", split_axis=0, concat_axis=0, tiled=True
    ).reshape(slabs, width, 2, rows, planes)
    image = image.transpose(1, 2, 3, 0, 4).reshape(width, 2, rows, nz)
    image = lax.all_gather(image, "coil", axis=2, tiled=True).swapaxes(2, 3)
    mask = lax.all_gather(sample_mask.astype(bf16), "slab", axis=2, tiled=True)

    maps = coil_maps.reshape(coils, 2, planes, ny, slabs, width).transpose(4, 0, 5, 1, 2, 3)
    maps, image, mask = lax.optimization_barrier((maps, image, mask))
    maps = exchange(maps)

    data = kspace_data * sample_mask[:, None, :, :, None].astype(bf16)
    data = jnp.einsum("ckzyx,kjxw->cjzyw", data, inverse_x, preferred_element_type=f32).astype(bf16)
    data = jnp.einsum(
        "ckzyx,kjzw->cjywx", data, jnp.asarray(inverse_z), preferred_element_type=f32
    ).astype(bf16)
    data = data.reshape(coils, 2, shares, nz, slabs, width).transpose(4, 0, 5, 1, 2, 3)
    data, maps = lax.optimization_barrier((data, maps))
    data = exchange(data)

    normal = apply_normal(image, maps, mask, tables)
    duals, spread = tv_update(image, None)
    data, normal, duals, spread = lax.optimization_barrier((data, normal, duals, spread))
    back_data = apply_data(data, maps, tables[3], image.shape)
    scale = dual_step / (1.0 + dual_step)
    data_grad = lax.psum(scale * (normal - back_data), "coil")
    updated = image - primal_step * (data_grad + spread)
    guess = 2.0 * updated - image
    normal = apply_normal(guess, maps, mask, tables)
    _, spread = tv_update(guess, duals)
    known = updated - primal_step * (data_grad / (1.0 + dual_step) + spread)
    share = known / groups - (primal_step * scale) * (normal - back_data)
    share = lax.psum_scatter(share.swapaxes(2, 3), "coil", scatter_dimension=2, tiled=True)
    share = share.reshape(width, 2, rows, slabs, planes).transpose(3, 1, 4, 2, 0)
    share = lax.all_to_all(
        share.reshape(slabs, -1), "slab", split_axis=0, concat_axis=0, tiled=True
    ).reshape(slabs, 2, planes, rows, width)
    return share.transpose(1, 2, 3, 0, 4).reshape(2, planes, rows, nx)


def solution(mesh):
    placed = (
        P("coil", None, None, "slab", None),
        P("coil", None, "slab", None, None),
        P("coil", None, "slab"),
        P(None, "slab", "coil", None),
    )
    return jax.shard_map(
        on_device,
        mesh=mesh,
        in_specs=placed,
        out_specs=P(None, "slab", "coil", None),
        check_vma=False,
    )
```
